32 devices in a mesh: tm: 16 (over z, x, core), chan: 2 (over y).
Axes of the slice: x: 2, y: 2, z: 4, core: 2. Of those that a mesh axis runs over, the one named last changes fastest.
Arguments:
- trans: float32 [4, 128, 32768], P(None, 'chan', 'tm'), may hold values from -1 to 1
- drive: float32 [2, 128, 32768], P(None, 'chan', 'tm'), may hold values from -60 to 60
- back_drive: float32 [2, 128, 32768], P(None, 'chan', 'tm'), may hold values from -60 to 60
- readout: float32 [128, 2, 128], P('chan'), may hold values from -0.375 to 0.375
Outputs:
- observed: float32 [128, 32768], P('chan', 'tm')
The draws below stay inside these ranges and needn't reach their ends.
All inputs are finite; a program needn't handle non-finite values.
Results may differ from the reference program's by a relative error of at most 0.0003.
Values sent between devices are 32-bit elements; how exact they have to be, the bound alone decides.
A program may use at most 64 MiB of HBM per device.

```python
import math
import jax
import jax.numpy as jnp
from jax import lax

CH = 128
TS_DEV = 2048
TOTAL_TIMESTEPS = 32768


def draw_trans(key, part):
    share = 0.5
    slow = jax.random.uniform(jax.random.fold_in(key, 1), (CH,)) < share
    slow_rate = 0.6 / TOTAL_TIMESTEPS * jnp.exp(jax.random.uniform(jax.random.fold_in(key, 2), (CH,), jnp.float32, -0.3, 0.3))
    fast_rate = 1.0 / jax.random.uniform(jax.random.fold_in(key, 3), (CH,), jnp.float32, 30.0, 50.0)
    base_level = jnp.where(slow, slow_rate, fast_rate)[:, None]
    block_count = TOTAL_TIMESTEPS // TS_DEV
    block_factor = jnp.exp(jax.random.uniform(jax.random.fold_in(key, 4), (CH, block_count), jnp.float32, math.log(0.5), math.log(2.0)))
    block_complete = jnp.repeat(block_factor, TS_DEV, axis=1)
    per_step_multiplier = jax.random.uniform(jax.random.fold_in(key, 5), (CH, TOTAL_TIMESTEPS), jnp.float32, 0.5, 1.5)
    spike_locations = jax.random.randint(jax.random.fold_in(key, 6), (3,), 0, TOTAL_TIMESTEPS)
    step_positions = jnp.arange(TOTAL_TIMESTEPS)
    spike_events = jnp.sum((step_positions[None, :] == spike_locations[:, None]).astype(jnp.float32), axis=0) * 0.5
    decay_factor = base_level * block_complete * per_step_multiplier + spike_events[None, :]
    scale = jnp.exp(-decay_factor)
    angle = jax.random.uniform(jax.random.fold_in(key, 7), (CH, TOTAL_TIMESTEPS), jnp.float32, -math.pi, math.pi)
    cosine = scale * jnp.cos(angle)
    sine = scale * jnp.sin(angle)
    return jnp.stack([cosine, -sine, sine, cosine], axis=0).astype(jnp.float32)


def common_drive(key):
    ramp = 1.0 + 2.0 * jnp.arange(TOTAL_TIMESTEPS).astype(jnp.float32) / (TOTAL_TIMESTEPS - 1)
    values = jax.random.truncated_normal(jax.random.fold_in(key, 3), -5.0, 5.0, (2, CH, TOTAL_TIMESTEPS), jnp.float32)
    return (values * ramp[None, None, :]).astype(jnp.float32)


def draw_drive(key, part):
    return common_drive(jax.random.fold_in(key, 11))


def draw_back_drive(key, part):
    return common_drive(jax.random.fold_in(key, 12))


def shard_levels(stream_key, extent, pieces, least, largest):
    gain = 1.0
    for position, parts in pieces:
        draws = jax.random.uniform(jax.random.fold_in(jax.random.fold_in(stream_key, 6), position), (parts,), jnp.float32, least / len(pieces), largest / len(pieces))
        gain = gain * jnp.repeat(jnp.exp(draws), extent[position] // parts).reshape((-1,) + (1,) * (len(extent) - 1 - position))
    return gain


def bell_draw(key, dims, scale, most, cuts=(), kind=jnp.bfloat16):
    values = scale * jax.random.normal(key, dims, jnp.float32)
    if cuts:
        values = values * shard_levels(key, dims, cuts, -0.22, 0.18)
    return jnp.clip(values, -most, most).astype(kind)


def setup_inputs(seed: int = 0) -> dict:
    arg_keys = jax.random.split(jax.random.key(seed), 5)
    return {
        "trans": draw_trans(jax.random.fold_in(arg_keys[4], 71), 0),
        "drive": draw_drive(jax.random.fold_in(arg_keys[4], 71), 0),
        "back_drive": draw_back_drive(jax.random.fold_in(arg_keys[4], 71), 0),
        "readout": bell_draw(arg_keys[3], (CH, 2, CH), (2 * CH) ** -0.5, 0.375, ((0, 2),), jnp.float32),
    }


epsilon = 1e-06

def forward_step(state, inputs):
    matrix, source = inputs
    first = matrix[0] * state[0] + matrix[1] * state[1] + source[0]
    second = matrix[2] * state[0] + matrix[3] * state[1] + source[1]
    result = jnp.stack([first, second], axis=0)
    return (result, result)

def backward_step(state, inputs):
    matrix, source = inputs
    first = matrix[0] * state[0] + matrix[2] * state[1] + source[0]
    second = matrix[1] * state[0] + matrix[3] * state[1] + source[1]
    result = jnp.stack([first, second], axis=0)
    return (result, result)

def reference(trans, drive, back_drive, readout):
    matrices = jnp.moveaxis(trans, 2, 0)
    sources = jnp.moveaxis(drive, 2, 0)
    back_sources = jnp.moveaxis(back_drive, 2, 0)
    start = jnp.zeros((2, CH), trans.dtype)
    _, forward_states = lax.scan(forward_step, start, (matrices, sources))
    _, backward_states = lax.scan(backward_step, start, (matrices, back_sources), reverse=True)
    count = 2.0 * TOTAL_TIMESTEPS
    norm_f = jnp.sqrt(lax.optimization_barrier(jnp.sum(forward_states * forward_states, axis=(0, 1))) / count + epsilon)
    norm_b = jnp.sqrt(lax.optimization_barrier(jnp.sum(backward_states * backward_states, axis=(0, 1))) / count + epsilon)
    smoothed = forward_states / norm_f + backward_states / norm_b
    smoothed = jnp.moveaxis(smoothed, 0, 2).reshape(2 * CH, TOTAL_TIMESTEPS)
    return jnp.dot(readout.reshape(CH, 2 * CH), smoothed, precision=lax.Precision.HIGHEST, preferred_element_type=jnp.float32)
```

```python
import functools

import jax
import jax.numpy as jnp
from jax import lax
from jax.experimental import pallas as pl
from jax.experimental.pallas import tpu as pltpu
from jax.sharding import PartitionSpec as P

MESH = pl.DeviceIdType.MESH
epsilon = 1e-06
LANES = 128
ROWS = 8


def cmul(ar, ai, br, bi):
    return ar * br - ai * bi, ar * bi + ai * br


def lane_total(value, width):
    shift = width
    while shift < LANES:
        value = value + pltpu.roll(value, shift, 1)
        shift *= 2
    return value


def chunk_prefix(maps, width, reverse):
    zr, zi, fr, fi = maps
    one = jnp.ones((1, LANES), jnp.float32)
    nil = jnp.zeros((1, LANES), jnp.float32)
    state = (one, nil, nil, nil)
    ahead = [None] * ROWS
    for k in range(ROWS - 1, -1, -1) if reverse else range(ROWS):
        ahead[k] = state
        pr, pi, ur, ui = state
        kr, ki = zr[k : k + 1], zi[k : k + 1]
        pr, pi = cmul(kr, ki, pr, pi)
        ur, ui = cmul(kr, ki, ur, ui)
        state = (pr, pi, ur + fr[k : k + 1], ui + fi[k : k + 1])
    rows = [jnp.concatenate([a[i] for a in ahead], axis=0) for i in range(4)]
    total = [jnp.broadcast_to(a, (ROWS, LANES)) for a in state]
    lane = lax.broadcasted_iota(jnp.int32, (ROWS, LANES), 1)
    if reverse:
        shift, edge, last = LANES - width, lane >= LANES - width, lane < width
    else:
        shift, edge, last = width, lane < width, lane >= LANES - width
    blocks = LANES // width

    def exclusive(inc):
        if blocks == 1:
            return [jnp.full((ROWS, LANES), e, jnp.float32) for e in (1.0, 0.0, 0.0, 0.0)]
        return [
            jnp.where(edge, e, pltpu.roll(a, shift, 1)) for a, e in zip(inc, (1.0, 0.0, 0.0, 0.0))
        ]

    inc = total
    for _ in range(blocks - 1):
        er, ei, gr, gi = exclusive(inc)
        er, ei = cmul(total[0], total[1], er, ei)
        gr, gi = cmul(total[0], total[1], gr, gi)
        inc = [er, ei, gr + total[2], gi + total[3]]
    er, ei, gr, gi = exclusive(inc)
    pr, pi = cmul(rows[0], rows[1], er, ei)
    ur, ui = cmul(rows[0], rows[1], gr, gi)
    whole = [lane_total(jnp.where(last, a, 0.0), width) for a in inc]
    return (pr, pi, ur + rows[2], ui + rows[3]), whole


def device_row(ahead, whole, sums, width):
    pr, pi, ur, ui = ahead
    s0, s1r, s1i, s2 = sums
    d0 = s0 + 2.0 * (ur * s1r + ui * s1i) + (ur * ur + ui * ui) * s2
    d1r, d1i = cmul(pr, -pi, s1r + ur * s2, s1i + ui * s2)
    d2 = (pr * pr + pi * pi) * s2
    sums = [jnp.sum(a, axis=0, keepdims=True) for a in (d0, d1r, d1i, d2)]
    sums = lane_total(jnp.concatenate(sums + sums, axis=0), width)
    return jnp.concatenate([a[0:1] for a in whole] + [sums[0:4]], axis=0)


def split(value):
    high = value.astype(jnp.bfloat16)
    return high, (value - high.astype(jnp.float32)).astype(jnp.bfloat16)


def body(
    n_tm,
    n_ch,
    trans,
    drive,
    back,
    readout,
    out,
    raw,
    turned,
    scans,
    smooth,
    reads,
    weights,
    gath,
    sends,
    recvs,
    own,
    final,
    in_sem,
    read_in,
    read_send,
    read_recv,
    gath_send,
    gath_recv,
    part_send,
    part_recv,
    out_sem,
):
    width = trans.shape[1]
    steps = trans.shape[2]
    blocks = LANES // width
    span = steps // blocks
    length = span // ROWS
    pitch = length + ROWS
    tiles = span // LANES
    outs = readout.shape[0] // 2
    me = lax.axis_index("tm")
    group = lax.axis_index("chan")

    planes = (trans.at[0], trans.at[2], drive.at[0], drive.at[1], back.at[0], back.at[1])
    loads = [pltpu.make_async_copy(src, raw.at[i], in_sem.at[i]) for i, src in enumerate(planes)]
    for copy in loads:
        copy.start()
    read_copy = pltpu.make_async_copy(readout, reads.at[0], read_in)
    read_copy.start()

    barrier = pltpu.get_barrier_semaphore()
    for d in range(1, n_tm):
        pl.semaphore_signal(
            barrier, inc=1, device_id={"tm": lax.rem(me + d, n_tm)}, device_id_type=MESH
        )
    for d in range(1, n_ch):
        pl.semaphore_signal(
            barrier, inc=1, device_id={"chan": lax.rem(group + d, n_ch)}, device_id_type=MESH
        )

    for i, copy in enumerate(loads):
        copy.wait()
        for b in range(tiles):
            block = jnp.concatenate(
                [
                    raw[i, :, h * span + b * LANES : h * span + (b + 1) * LANES]
                    for h in range(blocks)
                ],
                axis=0,
            ).T
            for at in range(0, LANES, length):
                k = (b * LANES + at) // length
                turned[i, k * pitch : k * pitch + length, :] = block[at : at + length]

    read_copy.wait()
    pl.semaphore_wait(barrier, n_tm + n_ch - 2)
    read_sends = []
    for d in range(1, n_ch):
        copy = pltpu.make_async_remote_copy(
            src_ref=reads.at[0],
            dst_ref=reads.at[d],
            send_sem=read_send.at[d],
            recv_sem=read_recv.at[d],
            device_id={"chan": lax.rem(group + d, n_ch)},
            device_id_type=MESH,
        )
        copy.start()
        read_sends.append(copy)

    nil = jnp.zeros((ROWS, LANES), jnp.float32)
    one = jnp.ones((ROWS, LANES), jnp.float32)

    def advance(state, p, q, dr, di):
        fr, fi, ar, ai, s0, s1r, s1i, s2 = state
        fr, fi = p * fr - q * fi + dr, q * fr + p * fi + di
        ar, ai = p * ar - q * ai, q * ar + p * ai
        s0 = s0 + (fr * fr + fi * fi)
        s1r = s1r + (ar * fr + ai * fi)
        s1i = s1i + (ar * fi - ai * fr)
        s2 = s2 + (ar * ar + ai * ai)
        return fr, fi, ar, ai, s0, s1r, s1i, s2

    def scan_step(s, state):
        f, g = state
        rows = pl.ds(s, ROWS, stride=pitch)
        f = advance(
            f,
            turned.at[0][rows, :],
            turned.at[1][rows, :],
            turned.at[2][rows, :],
            turned.at[3][rows, :],
        )
        r = length - 1 - s
        rows = pl.ds(r, ROWS, stride=pitch)
        g = advance(
            g,
            turned.at[0][rows, :],
            -turned.at[1][rows, :],
            turned.at[4][rows, :],
            turned.at[5][rows, :],
        )
        for i in range(4):
            scans[i, s] = f[i]
            scans[4 + i, r] = g[i]
        return f, g

    start = (nil, nil, one, nil, nil, nil, nil, nil)
    f, g = lax.fori_loop(0, length, scan_step, (start, start), unroll=4)
    ahead_f, whole_f = chunk_prefix((f[2], f[3], f[0], f[1]), width, False)
    ahead_b, whole_b = chunk_prefix((g[2], g[3], g[0], g[1]), width, True)
    gath[0, 0:ROWS] = device_row(ahead_f, whole_f, f[4:], width)
    gath[0, ROWS : 2 * ROWS] = device_row(ahead_b, whole_b, g[4:], width)
    gath_copies = []
    for d in range(1, n_tm):
        copy = pltpu.make_async_remote_copy(
            src_ref=gath.at[0],
            dst_ref=gath.at[d],
            send_sem=gath_send.at[d],
            recv_sem=gath_recv.at[d],
            device_id={"tm": lax.rem(me + d, n_tm)},
            device_id_type=MESH,
        )
        copy.start()
        gath_copies.append(copy)

    for copy in read_sends:
        copy.wait()
    lane = lax.broadcasted_iota(jnp.int32, (outs, LANES), 1)
    for e in range(n_ch):
        slab = reads.at[(n_ch - e) % n_ch]
        for k in range(2):
            part = slab[pl.ds(k, outs, stride=2), :]
            for h in range(blocks):
                shift = lax.rem(h * width + LANES - group * width, LANES)
                moved = pltpu.roll(part, shift, 1)
                moved = jnp.where((lane >= h * width) & (lane < (h + 1) * width), moved, 0.0)
                high, low = split(moved)
                weights[e, 0, h * outs : (h + 1) * outs, k * LANES : (k + 1) * LANES] = high
                weights[e, 1, h * outs : (h + 1) * outs, k * LANES : (k + 1) * LANES] = low

    for copy in gath_copies:
        copy.wait()

    def along(order, base):
        zero = jnp.zeros((1, LANES), jnp.float32)
        cr, ci, keep_r, keep_i, norm = zero, zero, zero, zero, zero
        for j in order:
            stat = gath[lax.rem(me - j + n_tm, n_tm), base : base + ROWS]
            zr, zi, tr, ti, d0, d1r, d1i, d2 = [stat[i : i + 1] for i in range(ROWS)]
            mine = jnp.full((1, LANES), me, jnp.int32) == j
            keep_r = jnp.where(mine, cr, keep_r)
            keep_i = jnp.where(mine, ci, keep_i)
            norm = norm + (d0 + 2.0 * (cr * d1r + ci * d1i) + (cr * cr + ci * ci) * d2)
            cr, ci = zr * cr - zi * ci + tr, zr * ci + zi * cr + ti
        scale = 1.0 / jnp.sqrt(norm / (2.0 * steps * n_tm) + epsilon)
        return keep_r, keep_i, scale

    def carries(ahead, order, base):
        cr, ci, scale = along(order, base)
        pr, pi, ur, ui = ahead
        xr, xi = cmul(pr, pi, cr, ci)
        return (xr + ur) * scale, (xi + ui) * scale, jnp.broadcast_to(scale, (ROWS, LANES))

    cr, ci, cs = carries(ahead_f, range(n_tm), 0)
    dr, di, ds = carries(ahead_b, range(n_tm - 1, -1, -1), ROWS)

    def smooth_step(s, _):
        fr, fi, ar, ai, gr, gi, br, bi = [scans[i, s] for i in range(8)]
        rows = pl.ds(s, ROWS, stride=pitch)
        smooth.at[0][rows, :] = (fr * cs + (ar * cr - ai * ci)) + (gr * ds + (br * dr - bi * di))
        smooth.at[1][rows, :] = (fi * cs + (ar * ci + ai * cr)) + (gi * ds + (br * di + bi * dr))
        return 0

    lax.fori_loop(0, length, smooth_step, 0, unroll=4)

    def tile_of(b):
        per = LANES // length if length < LANES else 1
        first = b * LANES // length
        offset = b * LANES - first * length
        size = min(length, LANES)
        return [
            jnp.concatenate(
                [
                    smooth[c, (first + i) * pitch + offset : (first + i) * pitch + offset + size, :]
                    for i in range(per)
                ],
                axis=0,
            )
            for c in range(2)
        ]

    def product(e, right):
        high, low = right
        dims = (((1,), (1,)), ((), ()))
        dot = functools.partial(
            lax.dot_general, dimension_numbers=dims, preferred_element_type=jnp.float32
        )
        return dot(weights[e, 0], high) + (dot(weights[e, 1], high) + dot(weights[e, 0], low))

    part_copies = {}
    rights = []
    for b in range(tiles):
        right = split(jnp.concatenate(tile_of(b), axis=1))
        rights.append(right)
        for e in range(1, n_ch):
            sends[e - 1, b] = product(e, right)
            copy = pltpu.make_async_remote_copy(
                src_ref=sends.at[e - 1, b],
                dst_ref=recvs.at[e - 1, b],
                send_sem=part_send.at[e - 1, b],
                recv_sem=part_recv.at[e - 1, b],
                device_id={"chan": lax.rem(group + e, n_ch)},
                device_id_type=MESH,
            )
            copy.start()
            part_copies[e, b] = copy
    for b in range(tiles):
        right = split(jnp.concatenate(tile_of(b), axis=1))
        own[b] = product(0, right)
    out_copies = []
    for b in range(tiles):
        total = own[b]
        for e in range(1, n_ch):
            part_copies[e, b].wait_recv()
            total = total + recvs[e - 1, b]
        for h in range(blocks):
            at = h * span + b * LANES
            final[:, at : at + LANES] = total[h * outs : (h + 1) * outs]
            copy = pltpu.make_async_copy(
                final.at[:, at : at + LANES], out.at[:, at : at + LANES], out_sem.at[b, h]
            )
            copy.start()
            out_copies.append(copy)
    for copy in part_copies.values():
        copy.wait_send()
    for copy in out_copies:
        copy.wait()


def on_device(n_tm, n_ch, trans, drive, back_drive, readout):
    width, steps = trans.shape[1], trans.shape[2]
    outs = readout.shape[0]
    blocks = LANES // width
    span = steps // blocks
    length = span // ROWS
    pitch = length + ROWS
    tiles = span // LANES
    f32 = jnp.float32
    dma = pltpu.SemaphoreType.DMA
    any_space = pl.BlockSpec(memory_space=pl.ANY)
    return pl.pallas_call(
        functools.partial(body, n_tm, n_ch),
        out_shape=jax.ShapeDtypeStruct((outs, steps), f32),
        in_specs=[any_space] * 4,
        out_specs=any_space,
        scratch_shapes=[
            pltpu.VMEM((6, width, steps), f32),
            pltpu.VMEM((6, ROWS * pitch, LANES), f32),
            pltpu.VMEM((8, length, ROWS, LANES), f32),
            pltpu.VMEM((2, ROWS * pitch, LANES), f32),
            pltpu.VMEM((n_ch, 2 * outs, LANES), f32),
            pltpu.VMEM((n_ch, 2, blocks * outs, 2 * LANES), jnp.bfloat16),
            pltpu.VMEM((n_tm, 2 * ROWS, LANES), f32),
            pltpu.VMEM((n_ch - 1, tiles, blocks * outs, LANES), f32),
            pltpu.VMEM((n_ch - 1, tiles, blocks * outs, LANES), f32),
            pltpu.VMEM((tiles, blocks * outs, LANES), f32),
            pltpu.VMEM((outs, steps), f32),
            dma((6,)),
            dma,
            dma((n_ch,)),
            dma((n_ch,)),
            dma((n_tm,)),
            dma((n_tm,)),
            dma((n_ch - 1, tiles)),
            dma((n_ch - 1, tiles)),
            dma((tiles, blocks)),
        ],
        compiler_params=pltpu.CompilerParams(
            collective_id=0, has_side_effects=True, vmem_limit_bytes=48 * 1024 * 1024
        ),
    )(trans, drive, back_drive, readout.reshape(2 * outs, readout.shape[2]))


def solution(mesh):
    in_specs = (
        P(None, "chan", "tm"),
        P(None, "chan", "tm"),
        P(None, "chan", "tm"),
        P("chan", None, None),
    )
    return jax.shard_map(
        functools.partial(on_device, mesh.shape["tm"], mesh.shape["chan"]),
        mesh=mesh,
        in_specs=in_specs,
        out_specs=P("chan", "tm"),
        check_vma=False,
    )
```

```python
import functools

import jax
import jax.numpy as jnp
from jax import lax
from jax.experimental import pallas as pl
from jax.experimental.pallas import tpu as pltpu
from jax.sharding import PartitionSpec as P

MESH = pl.DeviceIdType.MESH
epsilon = 1e-06
LANES = 128
ROWS = 8


def cmul(ar, ai, br, bi):
    return ar * br - ai * bi, ar * bi + ai * br


def lane_total(value, width):
    shift = width
    while shift < LANES:
        value = value + pltpu.roll(value, shift, 1)
        shift *= 2
    return value


def chunk_prefix(maps, width, reverse):
    zr, zi, fr, fi = maps
    one = jnp.ones((1, LANES), jnp.float32)
    nil = jnp.zeros((1, LANES), jnp.float32)
    state = (one, nil, nil, nil)
    ahead = [None] * ROWS
    for k in range(ROWS - 1, -1, -1) if reverse else range(ROWS):
        ahead[k] = state
        pr, pi, ur, ui = state
        kr, ki = zr[k : k + 1], zi[k : k + 1]
        pr, pi = cmul(kr, ki, pr, pi)
        ur, ui = cmul(kr, ki, ur, ui)
        state = (pr, pi, ur + fr[k : k + 1], ui + fi[k : k + 1])
    rows = [jnp.concatenate([a[i] for a in ahead], axis=0) for i in range(4)]
    total = [jnp.broadcast_to(a, (ROWS, LANES)) for a in state]
    lane = lax.broadcasted_iota(jnp.int32, (ROWS, LANES), 1)
    if reverse:
        shift, edge, last = LANES - width, lane >= LANES - width, lane < width
    else:
        shift, edge, last = width, lane < width, lane >= LANES - width
    blocks = LANES // width

    def exclusive(inc):
        if blocks == 1:
            return [jnp.full((ROWS, LANES), e, jnp.float32) for e in (1.0, 0.0, 0.0, 0.0)]
        return [
            jnp.where(edge, e, pltpu.roll(a, shift, 1)) for a, e in zip(inc, (1.0, 0.0, 0.0, 0.0))
        ]

    inc = total
    for _ in range(blocks - 1):
        er, ei, gr, gi = exclusive(inc)
        er, ei = cmul(total[0], total[1], er, ei)
        gr, gi = cmul(total[0], total[1], gr, gi)
        inc = [er, ei, gr + total[2], gi + total[3]]
    er, ei, gr, gi = exclusive(inc)
    pr, pi = cmul(rows[0], rows[1], er, ei)
    ur, ui = cmul(rows[0], rows[1], gr, gi)
    whole = [lane_total(jnp.where(last, a, 0.0), width) for a in inc]
    return (pr, pi, ur + rows[2], ui + rows[3]), whole


def device_row(ahead, whole, sums, width):
    pr, pi, ur, ui = ahead
    s0, s1r, s1i, s2 = sums
    d0 = s0 + 2.0 * (ur * s1r + ui * s1i) + (ur * ur + ui * ui) * s2
    d1r, d1i = cmul(pr, -pi, s1r + ur * s2, s1i + ui * s2)
    d2 = (pr * pr + pi * pi) * s2
    sums = [jnp.sum(a, axis=0, keepdims=True) for a in (d0, d1r, d1i, d2)]
    sums = lane_total(jnp.concatenate(sums + sums, axis=0), width)
    return jnp.concatenate([a[0:1] for a in whole] + [sums[0:4]], axis=0)


def split(value):
    high = value.astype(jnp.bfloat16)
    return high, (value - high.astype(jnp.float32)).astype(jnp.bfloat16)


def body(
    n_tm,
    n_ch,
    trans,
    drive,
    back,
    readout,
    out,
    raw,
    turned,
    scans,
    smooth,
    reads,
    weights,
    gath,
    sends,
    recvs,
    own,
    final,
    in_sem,
    read_in,
    read_send,
    read_recv,
    gath_send,
    gath_recv,
    part_send,
    part_recv,
    out_sem,
):
    width = trans.shape[1]
    steps = trans.shape[2]
    blocks = LANES // width
    span = steps // blocks
    length = span // ROWS
    pitch = length + ROWS
    tiles = span // LANES
    outs = readout.shape[0] // 2
    me = lax.axis_index("tm")
    group = lax.axis_index("chan")

    planes = (trans.at[0], trans.at[2], drive.at[0], drive.at[1], back.at[0], back.at[1])
    loads = [pltpu.make_async_copy(src, raw.at[i], in_sem.at[i]) for i, src in enumerate(planes)]
    for copy in loads:
        copy.start()
    read_copy = pltpu.make_async_copy(readout, reads.at[0], read_in)
    read_copy.start()

    barrier = pltpu.get_barrier_semaphore()
    for d in range(1, n_tm):
        pl.semaphore_signal(
            barrier, inc=1, device_id={"tm": lax.rem(me + d, n_tm)}, device_id_type=MESH
        )
    for d in range(1, n_ch):
        pl.semaphore_signal(
            barrier, inc=1, device_id={"chan": lax.rem(group + d, n_ch)}, device_id_type=MESH
        )

    read_sends = []
    for i, copy in enumerate(loads):
        copy.wait()
        for b in range(tiles):
            block = jnp.concatenate(
                [
                    raw[i, :, h * span + b * LANES : h * span + (b + 1) * LANES]
                    for h in range(blocks)
                ],
                axis=0,
            ).T
            for at in range(0, LANES, length):
                k = (b * LANES + at) // length
                turned[i, k * pitch : k * pitch + length, :] = block[at : at + length]

    read_copy.wait()
    pl.semaphore_wait(barrier, n_tm + n_ch - 2)
    for d in range(1, n_ch):
        copy = pltpu.make_async_remote_copy(
            src_ref=reads.at[0],
            dst_ref=reads.at[d],
            send_sem=read_send.at[d],
            recv_sem=read_recv.at[d],
            device_id={"chan": lax.rem(group + d, n_ch)},
            device_id_type=MESH,
        )
        copy.start()
        read_sends.append(copy)

    nil = jnp.zeros((ROWS, LANES), jnp.float32)
    one = jnp.ones((ROWS, LANES), jnp.float32)

    def advance(state, p, q, dr, di):
        fr, fi, ar, ai, s0, s1r, s1i, s2 = state
        fr, fi = p * fr - q * fi + dr, q * fr + p * fi + di
        ar, ai = p * ar - q * ai, q * ar + p * ai
        s0 = s0 + (fr * fr + fi * fi)
        s1r = s1r + (ar * fr + ai * fi)
        s1i = s1i + (ar * fi - ai * fr)
        s2 = s2 + (ar * ar + ai * ai)
        return fr, fi, ar, ai, s0, s1r, s1i, s2

    def scan_step(s, state):
        f, g = state
        rows = pl.ds(s, ROWS, stride=pitch)
        f = advance(
            f,
            turned.at[0][rows, :],
            turned.at[1][rows, :],
            turned.at[2][rows, :],
            turned.at[3][rows, :],
        )
        r = length - 1 - s
        rows = pl.ds(r, ROWS, stride=pitch)
        g = advance(
            g,
            turned.at[0][rows, :],
            -turned.at[1][rows, :],
            turned.at[4][rows, :],
            turned.at[5][rows, :],
        )
        for i in range(4):
            scans[i, s] = f[i]
            scans[4 + i, r] = g[i]
        return f, g

    start = (nil, nil, one, nil, nil, nil, nil, nil)
    f, g = lax.fori_loop(0, length, scan_step, (start, start), unroll=4)
    ahead_f, whole_f = chunk_prefix((f[2], f[3], f[0], f[1]), width, False)
    ahead_b, whole_b = chunk_prefix((g[2], g[3], g[0], g[1]), width, True)
    row_f = device_row(ahead_f, whole_f, f[4:], width)
    row_b = device_row(ahead_b, whole_b, g[4:], width)
    low = lax.broadcasted_iota(jnp.int32, (ROWS, LANES), 1) < LANES // 2
    gath[0] = jnp.where(low, row_f, row_b)
    gath_copies = []
    for d in range(1, n_tm):
        copy = pltpu.make_async_remote_copy(
            src_ref=gath.at[0],
            dst_ref=gath.at[d],
            send_sem=gath_send.at[d],
            recv_sem=gath_recv.at[d],
            device_id={"tm": lax.rem(me + d, n_tm)},
            device_id_type=MESH,
        )
        copy.start()
        gath_copies.append(copy)

    for copy in read_sends:
        copy.wait()
    lane = lax.broadcasted_iota(jnp.int32, (outs, LANES), 1)
    for e in range(n_ch):
        slab = reads.at[(n_ch - e) % n_ch]
        for k in range(2):
            part = slab[pl.ds(k, outs, stride=2), :]
            for h in range(blocks):
                shift = lax.rem(h * width + LANES - group * width, LANES)
                moved = pltpu.roll(part, shift, 1)
                moved = jnp.where((lane >= h * width) & (lane < (h + 1) * width), moved, 0.0)
                head, tail = split(moved)
                weights[e, 0, h * outs : (h + 1) * outs, k * LANES : (k + 1) * LANES] = head
                weights[e, 1, h * outs : (h + 1) * outs, k * LANES : (k + 1) * LANES] = tail

    for copy in gath_copies:
        copy.wait()

    zero = jnp.zeros((1, LANES), jnp.float32)
    low_row = lax.broadcasted_iota(jnp.int32, (1, LANES), 1) < LANES // 2
    place = jnp.where(low_row, me, n_tm - 1 - me)
    xr, xi, keep_r, keep_i, norm = zero, zero, zero, zero, zero
    for j in range(n_tm):
        stat = jnp.where(
            low,
            gath[lax.rem(me - j + n_tm, n_tm)],
            gath[lax.rem(me + j + 1, n_tm)],
        )
        zr, zi, tr, ti, d0, d1r, d1i, d2 = [stat[i : i + 1] for i in range(ROWS)]
        keep_r = jnp.where(place == j, xr, keep_r)
        keep_i = jnp.where(place == j, xi, keep_i)
        norm = norm + (d0 + 2.0 * (xr * d1r + xi * d1i) + (xr * xr + xi * xi) * d2)
        xr, xi = zr * xr - zi * xi + tr, zr * xi + zi * xr + ti
    scale = 1.0 / jnp.sqrt(norm / (2.0 * steps * n_tm) + epsilon)
    mine = [jnp.broadcast_to(a, (ROWS, LANES)) for a in (keep_r, keep_i, scale)]
    moved = [pltpu.roll(a, LANES // 2, 1) for a in mine]

    def carries(ahead, whole):
        kr, ki, by = whole
        pr, pi, ur, ui = ahead
        kr, ki = cmul(pr, pi, kr, ki)
        return (kr + ur) * by, (ki + ui) * by, by

    cr, ci, cs = carries(ahead_f, [jnp.where(low, a, b) for a, b in zip(mine, moved)])
    dr, di, ds = carries(ahead_b, [jnp.where(low, b, a) for a, b in zip(mine, moved)])

    def smooth_step(s, _):
        fr, fi, ar, ai, gr, gi, br, bi = [scans[i, s] for i in range(8)]
        rows = pl.ds(s, ROWS, stride=pitch)
        smooth.at[0][rows, :] = (fr * cs + (ar * cr - ai * ci)) + (gr * ds + (br * dr - bi * di))
        smooth.at[1][rows, :] = (fi * cs + (ar * ci + ai * cr)) + (gi * ds + (br * di + bi * dr))
        return 0

    lax.fori_loop(0, length, smooth_step, 0, unroll=4)

    def tile_of(b):
        per = LANES // length if length < LANES else 1
        first = b * LANES // length
        offset = b * LANES - first * length
        size = min(length, LANES)
        return [
            jnp.concatenate(
                [
                    smooth[c, (first + i) * pitch + offset : (first + i) * pitch + offset + size, :]
                    for i in range(per)
                ],
                axis=0,
            )
            for c in range(2)
        ]

    def product(e, right):
        high, low = right
        dims = (((1,), (1,)), ((), ()))
        dot = functools.partial(
            lax.dot_general, dimension_numbers=dims, preferred_element_type=jnp.float32
        )
        return dot(weights[e, 0], high) + (dot(weights[e, 1], high) + dot(weights[e, 0], low))

    part_copies = {}
    rights = []
    for b in range(tiles):
        right = split(jnp.concatenate(tile_of(b), axis=1))
        rights.append(right)
        for e in range(1, n_ch):
            sends[e - 1, b] = product(e, right)
            copy = pltpu.make_async_remote_copy(
                src_ref=sends.at[e - 1, b],
                dst_ref=recvs.at[e - 1, b],
                send_sem=part_send.at[e - 1, b],
                recv_sem=part_recv.at[e - 1, b],
                device_id={"chan": lax.rem(group + e, n_ch)},
                device_id_type=MESH,
            )
            copy.start()
            part_copies[e, b] = copy
    for b in range(tiles):
        right = split(jnp.concatenate(tile_of(b), axis=1))
        own[b] = product(0, right)
    out_copies = []
    for b in range(tiles):
        total = own[b]
        for e in range(1, n_ch):
            part_copies[e, b].wait_recv()
            total = total + recvs[e - 1, b]
        for h in range(blocks):
            at = h * span + b * LANES
            final[:, at : at + LANES] = total[h * outs : (h + 1) * outs]
            copy = pltpu.make_async_copy(
                final.at[:, at : at + LANES], out.at[:, at : at + LANES], out_sem.at[b, h]
            )
            copy.start()
            out_copies.append(copy)
    for copy in part_copies.values():
        copy.wait_send()
    for copy in out_copies:
        copy.wait()


def on_device(n_tm, n_ch, trans, drive, back_drive, readout):
    width, steps = trans.shape[1], trans.shape[2]
    outs = readout.shape[0]
    blocks = LANES // width
    span = steps // blocks
    length = span // ROWS
    pitch = length + ROWS
    tiles = span // LANES
    f32 = jnp.float32
    dma = pltpu.SemaphoreType.DMA
    any_space = pl.BlockSpec(memory_space=pl.ANY)
    return pl.pallas_call(
        functools.partial(body, n_tm, n_ch),
        out_shape=jax.ShapeDtypeStruct((outs, steps), f32),
        in_specs=[any_space] * 4,
        out_specs=any_space,
        scratch_shapes=[
            pltpu.VMEM((6, width, steps), f32),
            pltpu.VMEM((6, ROWS * pitch, LANES), f32),
            pltpu.VMEM((8, length, ROWS, LANES), f32),
            pltpu.VMEM((2, ROWS * pitch, LANES), f32),
            pltpu.VMEM((n_ch, 2 * outs, LANES), f32),
            pltpu.VMEM((n_ch, 2, blocks * outs, 2 * LANES), jnp.bfloat16),
            pltpu.VMEM((n_tm, ROWS, LANES), f32),
            pltpu.VMEM((n_ch - 1, tiles, blocks * outs, LANES), f32),
            pltpu.VMEM((n_ch - 1, tiles, blocks * outs, LANES), f32),
            pltpu.VMEM((tiles, blocks * outs, LANES), f32),
            pltpu.VMEM((outs, steps), f32),
            dma((6,)),
            dma,
            dma((n_ch,)),
            dma((n_ch,)),
            dma((n_tm,)),
            dma((n_tm,)),
            dma((n_ch - 1, tiles)),
            dma((n_ch - 1, tiles)),
            dma((tiles, blocks)),
        ],
        compiler_params=pltpu.CompilerParams(
            collective_id=0, has_side_effects=True, vmem_limit_bytes=67043328
        ),
    )(trans, drive, back_drive, readout.reshape(2 * outs, readout.shape[2]))


def solution(mesh):
    in_specs = (
        P(None, "chan", "tm"),
        P(None, "chan", "tm"),
        P(None, "chan", "tm"),
        P("chan", None, None),
    )
    return jax.shard_map(
        functools.partial(on_device, mesh.shape["tm"], mesh.shape["chan"]),
        mesh=mesh,
        in_specs=in_specs,
        out_specs=P("chan", "tm"),
        check_vma=False,
    )
```

```python
import functools

import jax
import jax.numpy as jnp
from jax import lax
from jax.experimental import pallas as pl
from jax.experimental.pallas import tpu as pltpu
from jax.sharding import PartitionSpec as P

MESH = pl.DeviceIdType.MESH
epsilon = 1e-06
LANES = 128
ROWS = 8


def cmul(ar, ai, br, bi):
    return ar * br - ai * bi, ar * bi + ai * br


def lane_total(value, width):
    shift = width
    while shift < LANES:
        value = value + pltpu.roll(value, shift, 1)
        shift *= 2
    return value


def chunk_prefix(maps, width, reverse):
    zr, zi, fr, fi = maps
    one = jnp.ones((1, LANES), jnp.float32)
    nil = jnp.zeros((1, LANES), jnp.float32)
    state = (one, nil, nil, nil)
    ahead = [None] * ROWS
    for k in range(ROWS - 1, -1, -1) if reverse else range(ROWS):
        ahead[k] = state
        pr, pi, ur, ui = state
        kr, ki = zr[k : k + 1], zi[k : k + 1]
        pr, pi = cmul(kr, ki, pr, pi)
        ur, ui = cmul(kr, ki, ur, ui)
        state = (pr, pi, ur + fr[k : k + 1], ui + fi[k : k + 1])
    rows = [jnp.concatenate([a[i] for a in ahead], axis=0) for i in range(4)]
    total = [jnp.broadcast_to(a, (ROWS, LANES)) for a in state]
    lane = lax.broadcasted_iota(jnp.int32, (ROWS, LANES), 1)
    if reverse:
        shift, edge, last = LANES - width, lane >= LANES - width, lane < width
    else:
        shift, edge, last = width, lane < width, lane >= LANES - width
    blocks = LANES // width

    def exclusive(inc):
        if blocks == 1:
            return [jnp.full((ROWS, LANES), e, jnp.float32) for e in (1.0, 0.0, 0.0, 0.0)]
        return [
            jnp.where(edge, e, pltpu.roll(a, shift, 1)) for a, e in zip(inc, (1.0, 0.0, 0.0, 0.0))
        ]

    inc = total
    for _ in range(blocks - 1):
        er, ei, gr, gi = exclusive(inc)
        er, ei = cmul(total[0], total[1], er, ei)
        gr, gi = cmul(total[0], total[1], gr, gi)
        inc = [er, ei, gr + total[2], gi + total[3]]
    er, ei, gr, gi = exclusive(inc)
    pr, pi = cmul(rows[0], rows[1], er, ei)
    ur, ui = cmul(rows[0], rows[1], gr, gi)
    whole = [lane_total(jnp.where(last, a, 0.0), width) for a in inc]
    return (pr, pi, ur + rows[2], ui + rows[3]), whole


def device_row(ahead, whole, sums, width):
    pr, pi, ur, ui = ahead
    s0, s1r, s1i, s2 = sums
    d0 = s0 + 2.0 * (ur * s1r + ui * s1i) + (ur * ur + ui * ui) * s2
    d1r, d1i = cmul(pr, -pi, s1r + ur * s2, s1i + ui * s2)
    d2 = (pr * pr + pi * pi) * s2
    sums = [jnp.sum(a, axis=0, keepdims=True) for a in (d0, d1r, d1i, d2)]
    sums = lane_total(jnp.concatenate(sums + sums, axis=0), width)
    return jnp.concatenate([a[0:1] for a in whole] + [sums[0:4]], axis=0)


def split(value):
    high = value.astype(jnp.bfloat16)
    return high, (value - high.astype(jnp.float32)).astype(jnp.bfloat16)


def body(
    n_tm,
    n_ch,
    trans,
    drive,
    back,
    readout,
    out,
    raw,
    turned,
    scans,
    rights,
    reads,
    weights,
    gath,
    sends,
    recvs,
    own,
    in_sem,
    read_in,
    read_send,
    read_recv,
    gath_send,
    gath_recv,
    part_send,
    part_recv,
):
    width = trans.shape[1]
    steps = trans.shape[2]
    blocks = LANES // width
    span = steps // blocks
    length = span // ROWS
    pitch = length + ROWS
    tiles = span // LANES
    outs = readout.shape[0] // 2
    me = lax.axis_index("tm")
    group = lax.axis_index("chan")

    planes = (trans.at[0], trans.at[2], drive.at[0], drive.at[1], back.at[0], back.at[1])
    loads = [pltpu.make_async_copy(src, raw.at[i], in_sem.at[i]) for i, src in enumerate(planes)]
    for copy in loads:
        copy.start()
    read_copy = pltpu.make_async_copy(readout, reads.at[0], read_in)
    read_copy.start()

    barrier = pltpu.get_barrier_semaphore()
    for d in range(1, n_tm):
        pl.semaphore_signal(
            barrier, inc=1, device_id={"tm": lax.rem(me + d, n_tm)}, device_id_type=MESH
        )
    for d in range(1, n_ch):
        pl.semaphore_signal(
            barrier, inc=1, device_id={"chan": lax.rem(group + d, n_ch)}, device_id_type=MESH
        )

    read_sends = []
    for i, copy in enumerate(loads):
        copy.wait()
        for b in range(tiles):
            block = jnp.concatenate(
                [
                    raw[i, :, h * span + b * LANES : h * span + (b + 1) * LANES]
                    for h in range(blocks)
                ],
                axis=0,
            ).T
            for at in range(0, LANES, length):
                k = (b * LANES + at) // length
                turned[i, k * pitch : k * pitch + length, :] = block[at : at + length]

    read_copy.wait()
    pl.semaphore_wait(barrier, n_tm + n_ch - 2)
    for d in range(1, n_ch):
        copy = pltpu.make_async_remote_copy(
            src_ref=reads.at[0],
            dst_ref=reads.at[d],
            send_sem=read_send.at[d],
            recv_sem=read_recv.at[d],
            device_id={"chan": lax.rem(group + d, n_ch)},
            device_id_type=MESH,
        )
        copy.start()
        read_sends.append(copy)

    nil = jnp.zeros((ROWS, LANES), jnp.float32)
    one = jnp.ones((ROWS, LANES), jnp.float32)

    def advance(state, p, q, dr, di):
        fr, fi, ar, ai, s0, s1r, s1i, s2 = state
        fr, fi = p * fr - q * fi + dr, q * fr + p * fi + di
        ar, ai = p * ar - q * ai, q * ar + p * ai
        s0 = s0 + (fr * fr + fi * fi)
        s1r = s1r + (ar * fr + ai * fi)
        s1i = s1i + (ar * fi - ai * fr)
        s2 = s2 + (ar * ar + ai * ai)
        return fr, fi, ar, ai, s0, s1r, s1i, s2

    def scan_step(s, state):
        f, g = state
        rows = pl.ds(s, ROWS, stride=pitch)
        f = advance(
            f,
            turned.at[0][rows, :],
            turned.at[1][rows, :],
            turned.at[2][rows, :],
            turned.at[3][rows, :],
        )
        r = length - 1 - s
        rows = pl.ds(r, ROWS, stride=pitch)
        g = advance(
            g,
            turned.at[0][rows, :],
            -turned.at[1][rows, :],
            turned.at[4][rows, :],
            turned.at[5][rows, :],
        )
        for i in range(4):
            scans[i, pl.ds(pl.multiple_of(s * ROWS, ROWS), ROWS), :] = f[i]
            scans[4 + i, pl.ds(pl.multiple_of(r * ROWS, ROWS), ROWS), :] = g[i]
        return f, g

    start = (nil, nil, one, nil, nil, nil, nil, nil)
    f, g = lax.fori_loop(0, length, scan_step, (start, start), unroll=4)
    ahead_f, whole_f = chunk_prefix((f[2], f[3], f[0], f[1]), width, False)
    ahead_b, whole_b = chunk_prefix((g[2], g[3], g[0], g[1]), width, True)
    row_f = device_row(ahead_f, whole_f, f[4:], width)
    row_b = device_row(ahead_b, whole_b, g[4:], width)
    low = lax.broadcasted_iota(jnp.int32, (ROWS, LANES), 1) < LANES // 2
    gath[0] = jnp.where(low, row_f, row_b)
    gath_copies = []
    for d in range(1, n_tm):
        copy = pltpu.make_async_remote_copy(
            src_ref=gath.at[0],
            dst_ref=gath.at[d],
            send_sem=gath_send.at[d],
            recv_sem=gath_recv.at[d],
            device_id={"tm": lax.rem(me + d, n_tm)},
            device_id_type=MESH,
        )
        copy.start()
        gath_copies.append(copy)

    for copy in read_sends:
        copy.wait()
    lane = lax.broadcasted_iota(jnp.int32, (outs, LANES), 1)
    for e in range(n_ch):
        slab = reads.at[(n_ch - e) % n_ch]
        for k in range(2):
            part = slab[pl.ds(k, outs, stride=2), :]
            for h in range(blocks):
                shift = lax.rem(h * width + LANES - group * width, LANES)
                moved = pltpu.roll(part, shift, 1)
                moved = jnp.where((lane >= h * width) & (lane < (h + 1) * width), moved, 0.0)
                head, tail = split(moved)
                weights[e, 0, h * outs : (h + 1) * outs, k * LANES : (k + 1) * LANES] = head
                weights[e, 1, h * outs : (h + 1) * outs, k * LANES : (k + 1) * LANES] = tail

    for copy in gath_copies:
        copy.wait()

    zero = jnp.zeros((1, LANES), jnp.float32)
    low_row = lax.broadcasted_iota(jnp.int32, (1, LANES), 1) < LANES // 2
    place = jnp.where(low_row, me, n_tm - 1 - me)
    xr, xi, keep_r, keep_i, norm = zero, zero, zero, zero, zero
    for j in range(n_tm):
        stat = jnp.where(
            low,
            gath[lax.rem(me - j + n_tm, n_tm)],
            gath[lax.rem(me + j + 1, n_tm)],
        )
        zr, zi, tr, ti, d0, d1r, d1i, d2 = [stat[i : i + 1] for i in range(ROWS)]
        keep_r = jnp.where(place == j, xr, keep_r)
        keep_i = jnp.where(place == j, xi, keep_i)
        norm = norm + (d0 + 2.0 * (xr * d1r + xi * d1i) + (xr * xr + xi * xi) * d2)
        xr, xi = zr * xr - zi * xi + tr, zr * xi + zi * xr + ti
    scale = 1.0 / jnp.sqrt(norm / (2.0 * steps * n_tm) + epsilon)
    mine = [jnp.broadcast_to(a, (ROWS, LANES)) for a in (keep_r, keep_i, scale)]
    moved = [pltpu.roll(a, LANES // 2, 1) for a in mine]

    def carries(ahead, whole):
        kr, ki, by = whole
        pr, pi, ur, ui = ahead
        kr, ki = cmul(pr, pi, kr, ki)
        return (kr + ur) * by, (ki + ui) * by, by

    cr, ci, cs = carries(ahead_f, [jnp.where(low, a, b) for a, b in zip(mine, moved)])
    dr, di, ds = carries(ahead_b, [jnp.where(low, b, a) for a, b in zip(mine, moved)])

    def tile_of(b):
        size = min(length, LANES)
        firsts, seconds = [], []
        for at in range(b * LANES, (b + 1) * LANES, size):
            k, offset = at // length, at % length
            rows = pl.ds(offset * ROWS + k, size, stride=ROWS)
            fr, fi, ar, ai, gr, gi, br, bi = [scans.at[i][rows, :] for i in range(8)]
            er, ei, es = cr[k : k + 1], ci[k : k + 1], cs[k : k + 1]
            hr, hi, hs = dr[k : k + 1], di[k : k + 1], ds[k : k + 1]
            firsts.append((fr * es + (ar * er - ai * ei)) + (gr * hs + (br * hr - bi * hi)))
            seconds.append((fi * es + (ar * ei + ai * er)) + (gi * hs + (br * hi + bi * hr)))
        return jnp.concatenate(
            [jnp.concatenate(firsts, axis=0), jnp.concatenate(seconds, axis=0)], axis=1
        )

    def product(e, b):
        high, low = rights[b, 0], rights[b, 1]
        dims = (((1,), (1,)), ((), ()))
        dot = functools.partial(
            lax.dot_general, dimension_numbers=dims, preferred_element_type=jnp.float32
        )
        return dot(weights[e, 0], high) + (dot(weights[e, 1], high) + dot(weights[e, 0], low))

    part_copies = {}
    for b in range(tiles):
        rights[b, 0], rights[b, 1] = split(tile_of(b))
        for e in range(1, n_ch):
            sends[e - 1, b] = product(e, b)
            copy = pltpu.make_async_remote_copy(
                src_ref=sends.at[e - 1, b],
                dst_ref=recvs.at[e - 1, b],
                send_sem=part_send.at[e - 1, b],
                recv_sem=part_recv.at[e - 1, b],
                device_id={"chan": lax.rem(group + e, n_ch)},
                device_id_type=MESH,
            )
            copy.start()
            part_copies[e, b] = copy
    for b in range(tiles):
        own[b] = product(0, b)
    for b in range(tiles):
        total = own[b]
        for e in range(1, n_ch):
            part_copies[e, b].wait_recv()
            total = total + recvs[e - 1, b]
        for h in range(blocks):
            at = h * span + b * LANES
            out[:, at : at + LANES] = total[h * outs : (h + 1) * outs]
    for copy in part_copies.values():
        copy.wait_send()


def on_device(n_tm, n_ch, trans, drive, back_drive, readout):
    width, steps = trans.shape[1], trans.shape[2]
    outs = readout.shape[0]
    blocks = LANES // width
    span = steps // blocks
    length = span // ROWS
    pitch = length + ROWS
    tiles = span // LANES
    f32 = jnp.float32
    dma = pltpu.SemaphoreType.DMA
    far = pl.BlockSpec(memory_space=pl.ANY)
    return pl.pallas_call(
        functools.partial(body, n_tm, n_ch),
        out_shape=pltpu.VMEM((outs, steps), f32),
        in_specs=[far] * 4,
        out_specs=pl.BlockSpec(memory_space=pltpu.VMEM),
        scratch_shapes=[
            pltpu.VMEM((6, width, steps), f32),
            pltpu.VMEM((6, ROWS * pitch, LANES), f32),
            pltpu.VMEM((8, length * ROWS, LANES), f32),
            pltpu.VMEM((tiles, 2, LANES, 2 * LANES), jnp.bfloat16),
            pltpu.VMEM((n_ch, 2 * outs, LANES), f32),
            pltpu.VMEM((n_ch, 2, blocks * outs, 2 * LANES), jnp.bfloat16),
            pltpu.VMEM((n_tm, ROWS, LANES), f32),
            pltpu.VMEM((n_ch - 1, tiles, blocks * outs, LANES), f32),
            pltpu.VMEM((n_ch - 1, tiles, blocks * outs, LANES), f32),
            pltpu.VMEM((tiles, blocks * outs, LANES), f32),
            dma((6,)),
            dma,
            dma((n_ch,)),
            dma((n_ch,)),
            dma((n_tm,)),
            dma((n_tm,)),
            dma((n_ch - 1, tiles)),
            dma((n_ch - 1, tiles)),
        ],
        compiler_params=pltpu.CompilerParams(
            collective_id=0, has_side_effects=True, vmem_limit_bytes=67043328 - 4 * outs * steps
        ),
    )(trans, drive, back_drive, readout.reshape(2 * outs, readout.shape[2]))


def solution(mesh):
    in_specs = (
        P(None, "chan", "tm"),
        P(None, "chan", "tm"),
        P(None, "chan", "tm"),
        P("chan", None, None),
    )
    return jax.shard_map(
        functools.partial(on_device, mesh.shape["tm"], mesh.shape["chan"]),
        mesh=mesh,
        in_specs=in_specs,
        out_specs=P("chan", "tm"),
        check_vma=False,
    )
```

```python
import functools

import jax
import jax.numpy as jnp
from jax import lax
from jax.experimental import pallas as pl
from jax.experimental.pallas import tpu as pltpu
from jax.sharding import PartitionSpec as P

MESH = pl.DeviceIdType.MESH
epsilon = 1e-06
LANES = 128
ROWS = 8


def cmul(ar, ai, br, bi):
    return ar * br - ai * bi, ar * bi + ai * br


def lane_total(value, width):
    shift = width
    while shift < LANES:
        value = value + pltpu.roll(value, shift, 1)
        shift *= 2
    return value


def chunk_prefix(maps, width, reverse):
    zr, zi, fr, fi = maps
    one = jnp.ones((1, LANES), jnp.float32)
    nil = jnp.zeros((1, LANES), jnp.float32)
    state = (one, nil, nil, nil)
    ahead = [None] * ROWS
    for k in range(ROWS - 1, -1, -1) if reverse else range(ROWS):
        ahead[k] = state
        pr, pi, ur, ui = state
        kr, ki = zr[k : k + 1], zi[k : k + 1]
        pr, pi = cmul(kr, ki, pr, pi)
        ur, ui = cmul(kr, ki, ur, ui)
        state = (pr, pi, ur + fr[k : k + 1], ui + fi[k : k + 1])
    rows = [jnp.concatenate([a[i] for a in ahead], axis=0) for i in range(4)]
    total = [jnp.broadcast_to(a, (ROWS, LANES)) for a in state]
    lane = lax.broadcasted_iota(jnp.int32, (ROWS, LANES), 1)
    if reverse:
        shift, edge, last = LANES - width, lane >= LANES - width, lane < width
    else:
        shift, edge, last = width, lane < width, lane >= LANES - width
    blocks = LANES // width

    def exclusive(inc):
        if blocks == 1:
            return [jnp.full((ROWS, LANES), e, jnp.float32) for e in (1.0, 0.0, 0.0, 0.0)]
        return [
            jnp.where(edge, e, pltpu.roll(a, shift, 1)) for a, e in zip(inc, (1.0, 0.0, 0.0, 0.0))
        ]

    inc = total
    for _ in range(blocks - 1):
        er, ei, gr, gi = exclusive(inc)
        er, ei = cmul(total[0], total[1], er, ei)
        gr, gi = cmul(total[0], total[1], gr, gi)
        inc = [er, ei, gr + total[2], gi + total[3]]
    er, ei, gr, gi = exclusive(inc)
    pr, pi = cmul(rows[0], rows[1], er, ei)
    ur, ui = cmul(rows[0], rows[1], gr, gi)
    whole = [lane_total(jnp.where(last, a, 0.0), width) for a in inc]
    return (pr, pi, ur + rows[2], ui + rows[3]), whole


def device_row(ahead, whole, sums, width):
    pr, pi, ur, ui = ahead
    s0, s1r, s1i, s2 = sums
    d0 = s0 + 2.0 * (ur * s1r + ui * s1i) + (ur * ur + ui * ui) * s2
    d1r, d1i = cmul(pr, -pi, s1r + ur * s2, s1i + ui * s2)
    d2 = (pr * pr + pi * pi) * s2
    sums = [jnp.sum(a, axis=0, keepdims=True) for a in (d0, d1r, d1i, d2)]
    sums = lane_total(jnp.concatenate(sums + sums, axis=0), width)
    return jnp.concatenate([a[0:1] for a in whole] + [sums[0:4]], axis=0)


def split(value):
    high = value.astype(jnp.bfloat16)
    return high, (value - high.astype(jnp.float32)).astype(jnp.bfloat16)


def body(
    n_tm,
    n_ch,
    trans,
    drive,
    back,
    readout,
    out,
    raw,
    turned,
    scans,
    rights,
    reads,
    weights,
    gath,
    sends,
    recvs,
    own,
    in_sem,
    read_in,
    read_send,
    read_recv,
    gath_send,
    gath_recv,
    part_send,
    part_recv,
):
    width = trans.shape[1]
    steps = trans.shape[2]
    blocks = LANES // width
    span = steps // blocks
    length = span // ROWS
    pitch = length + ROWS
    tiles = span // LANES
    outs = readout.shape[0] // 2
    me = lax.axis_index("tm")
    group = lax.axis_index("chan")

    planes = (trans.at[0], trans.at[2], drive.at[0], drive.at[1], back.at[0], back.at[1])
    loads = [pltpu.make_async_copy(src, raw.at[i], in_sem.at[i]) for i, src in enumerate(planes)]
    read_copy = pltpu.make_async_copy(readout, reads.at[0], read_in)
    read_copy.start()
    for copy in loads:
        copy.start()

    barrier = pltpu.get_barrier_semaphore()
    for d in range(1, n_tm):
        pl.semaphore_signal(
            barrier, inc=1, device_id={"tm": lax.rem(me + d, n_tm)}, device_id_type=MESH
        )
    for d in range(1, n_ch):
        pl.semaphore_signal(
            barrier, inc=1, device_id={"chan": lax.rem(group + d, n_ch)}, device_id_type=MESH
        )

    read_sends = []
    for i, copy in enumerate(loads):
        copy.wait()
        for b in range(tiles):
            block = jnp.concatenate(
                [
                    raw[i, :, h * span + b * LANES : h * span + (b + 1) * LANES]
                    for h in range(blocks)
                ],
                axis=0,
            ).T
            for at in range(0, LANES, length):
                k = (b * LANES + at) // length
                turned[i, k * pitch : k * pitch + length, :] = block[at : at + length]

    read_copy.wait()
    pl.semaphore_wait(barrier, n_tm + n_ch - 2)
    for d in range(1, n_ch):
        copy = pltpu.make_async_remote_copy(
            src_ref=reads.at[0],
            dst_ref=reads.at[d],
            send_sem=read_send.at[d],
            recv_sem=read_recv.at[d],
            device_id={"chan": lax.rem(group + d, n_ch)},
            device_id_type=MESH,
        )
        copy.start()
        read_sends.append(copy)

    nil = jnp.zeros((ROWS, LANES), jnp.float32)
    one = jnp.ones((ROWS, LANES), jnp.float32)

    def advance(state, p, q, dr, di):
        fr, fi, ar, ai, s0, s1r, s1i, s2 = state
        fr, fi = p * fr - q * fi + dr, q * fr + p * fi + di
        ar, ai = p * ar - q * ai, q * ar + p * ai
        s0 = s0 + (fr * fr + fi * fi)
        s1r = s1r + (ar * fr + ai * fi)
        s1i = s1i + (ar * fi - ai * fr)
        s2 = s2 + (ar * ar + ai * ai)
        return fr, fi, ar, ai, s0, s1r, s1i, s2

    def scan_step(s, state):
        f, g = state
        rows = pl.ds(s, ROWS, stride=pitch)
        f = advance(
            f,
            turned.at[0][rows, :],
            turned.at[1][rows, :],
            turned.at[2][rows, :],
            turned.at[3][rows, :],
        )
        r = length - 1 - s
        rows = pl.ds(r, ROWS, stride=pitch)
        g = advance(
            g,
            turned.at[0][rows, :],
            -turned.at[1][rows, :],
            turned.at[4][rows, :],
            turned.at[5][rows, :],
        )
        for i in range(4):
            scans[i, pl.ds(pl.multiple_of(s * ROWS, ROWS), ROWS), :] = f[i]
            scans[4 + i, pl.ds(pl.multiple_of(r * ROWS, ROWS), ROWS), :] = g[i]
        return f, g

    start = (nil, nil, one, nil, nil, nil, nil, nil)
    f, g = lax.fori_loop(0, length, scan_step, (start, start), unroll=4)
    ahead_f, whole_f = chunk_prefix((f[2], f[3], f[0], f[1]), width, False)
    ahead_b, whole_b = chunk_prefix((g[2], g[3], g[0], g[1]), width, True)
    row_f = device_row(ahead_f, whole_f, f[4:], width)
    row_b = device_row(ahead_b, whole_b, g[4:], width)
    low = lax.broadcasted_iota(jnp.int32, (ROWS, LANES), 1) < LANES // 2
    gath[0] = jnp.where(low, row_f, row_b)
    gath_copies = []
    for d in sorted(range(1, n_tm), key=lambda d: -min(d, n_tm - d)):
        copy = pltpu.make_async_remote_copy(
            src_ref=gath.at[0],
            dst_ref=gath.at[d],
            send_sem=gath_send.at[d],
            recv_sem=gath_recv.at[d],
            device_id={"tm": lax.rem(me + d, n_tm)},
            device_id_type=MESH,
        )
        copy.start()
        gath_copies.append(copy)

    for copy in read_sends:
        copy.wait()
    lane = lax.broadcasted_iota(jnp.int32, (outs, LANES), 1)
    for e in range(n_ch):
        slab = reads.at[(n_ch - e) % n_ch]
        for k in range(2):
            part = slab[pl.ds(k, outs, stride=2), :]
            for h in range(blocks):
                shift = lax.rem(h * width + LANES - group * width, LANES)
                moved = pltpu.roll(part, shift, 1)
                moved = jnp.where((lane >= h * width) & (lane < (h + 1) * width), moved, 0.0)
                head, tail = split(moved)
                weights[e, 0, h * outs : (h + 1) * outs, k * LANES : (k + 1) * LANES] = head
                weights[e, 1, h * outs : (h + 1) * outs, k * LANES : (k + 1) * LANES] = tail

    for copy in gath_copies:
        copy.wait()

    zero = jnp.zeros((1, LANES), jnp.float32)
    low_row = lax.broadcasted_iota(jnp.int32, (1, LANES), 1) < LANES // 2
    place = jnp.where(low_row, me, n_tm - 1 - me)
    xr, xi, keep_r, keep_i, norm = zero, zero, zero, zero, zero
    for j in range(n_tm):
        stat = jnp.where(
            low,
            gath[lax.rem(me - j + n_tm, n_tm)],
            gath[lax.rem(me + j + 1, n_tm)],
        )
        zr, zi, tr, ti, d0, d1r, d1i, d2 = [stat[i : i + 1] for i in range(ROWS)]
        keep_r = jnp.where(place == j, xr, keep_r)
        keep_i = jnp.where(place == j, xi, keep_i)
        norm = norm + (d0 + 2.0 * (xr * d1r + xi * d1i) + (xr * xr + xi * xi) * d2)
        xr, xi = zr * xr - zi * xi + tr, zr * xi + zi * xr + ti
    scale = 1.0 / jnp.sqrt(norm / (2.0 * steps * n_tm) + epsilon)
    mine = [jnp.broadcast_to(a, (ROWS, LANES)) for a in (keep_r, keep_i, scale)]
    moved = [pltpu.roll(a, LANES // 2, 1) for a in mine]

    def carries(ahead, whole):
        kr, ki, by = whole
        pr, pi, ur, ui = ahead
        kr, ki = cmul(pr, pi, kr, ki)
        return (kr + ur) * by, (ki + ui) * by, by

    cr, ci, cs = carries(ahead_f, [jnp.where(low, a, b) for a, b in zip(mine, moved)])
    dr, di, ds = carries(ahead_b, [jnp.where(low, b, a) for a, b in zip(mine, moved)])

    def tile_of(b):
        size = min(length, LANES)
        firsts, seconds = [], []
        for at in range(b * LANES, (b + 1) * LANES, size):
            k, offset = at // length, at % length
            rows = pl.ds(offset * ROWS + k, size, stride=ROWS)
            fr, fi, ar, ai, gr, gi, br, bi = [scans.at[i][rows, :] for i in range(8)]
            er, ei, es = cr[k : k + 1], ci[k : k + 1], cs[k : k + 1]
            hr, hi, hs = dr[k : k + 1], di[k : k + 1], ds[k : k + 1]
            firsts.append((fr * es + (ar * er - ai * ei)) + (gr * hs + (br * hr - bi * hi)))
            seconds.append((fi * es + (ar * ei + ai * er)) + (gi * hs + (br * hi + bi * hr)))
        return jnp.concatenate(
            [jnp.concatenate(firsts, axis=0), jnp.concatenate(seconds, axis=0)], axis=1
        )

    def product(e, b):
        high, low = rights[b, 0], rights[b, 1]
        dims = (((1,), (1,)), ((), ()))
        dot = functools.partial(
            lax.dot_general, dimension_numbers=dims, preferred_element_type=jnp.float32
        )
        both = dot(weights[e].reshape(-1, 2 * LANES), high)
        count = blocks * outs
        return both[:count] + (both[count:] + dot(weights[e, 0], low))

    part_copies = {}
    for b in range(tiles):
        rights[b, 0], rights[b, 1] = split(tile_of(b))
        for e in range(1, n_ch):
            sends[e - 1, b] = product(e, b)
            copy = pltpu.make_async_remote_copy(
                src_ref=sends.at[e - 1, b],
                dst_ref=recvs.at[e - 1, b],
                send_sem=part_send.at[e - 1, b],
                recv_sem=part_recv.at[e - 1, b],
                device_id={"chan": lax.rem(group + e, n_ch)},
                device_id_type=MESH,
            )
            copy.start()
            part_copies[e, b] = copy
    for b in range(tiles):
        own[b] = product(0, b)
    for b in range(tiles):
        total = own[b]
        for e in range(1, n_ch):
            part_copies[e, b].wait_recv()
            total = total + recvs[e - 1, b]
        for h in range(blocks):
            at = h * span + b * LANES
            out[:, at : at + LANES] = total[h * outs : (h + 1) * outs]
    for copy in part_copies.values():
        copy.wait_send()


def on_device(n_tm, n_ch, trans, drive, back_drive, readout):
    width, steps = trans.shape[1], trans.shape[2]
    outs = readout.shape[0]
    blocks = LANES // width
    span = steps // blocks
    length = span // ROWS
    pitch = length + ROWS
    tiles = span // LANES
    f32 = jnp.float32
    dma = pltpu.SemaphoreType.DMA
    far = pl.BlockSpec(memory_space=pl.ANY)
    return pl.pallas_call(
        functools.partial(body, n_tm, n_ch),
        out_shape=pltpu.VMEM((outs, steps), f32),
        in_specs=[far] * 4,
        out_specs=pl.BlockSpec(memory_space=pltpu.VMEM),
        scratch_shapes=[
            pltpu.VMEM((6, width, steps), f32),
            pltpu.VMEM((6, ROWS * pitch, LANES), f32),
            pltpu.VMEM((8, length * ROWS, LANES), f32),
            pltpu.VMEM((tiles, 2, LANES, 2 * LANES), jnp.bfloat16),
            pltpu.VMEM((n_ch, 2 * outs, LANES), f32),
            pltpu.VMEM((n_ch, 2, blocks * outs, 2 * LANES), jnp.bfloat16),
            pltpu.VMEM((n_tm, ROWS, LANES), f32),
            pltpu.VMEM((n_ch - 1, tiles, blocks * outs, LANES), f32),
            pltpu.VMEM((n_ch - 1, tiles, blocks * outs, LANES), f32),
            pltpu.VMEM((tiles, blocks * outs, LANES), f32),
            dma((6,)),
            dma,
            dma((n_ch,)),
            dma((n_ch,)),
            dma((n_tm,)),
            dma((n_tm,)),
            dma((n_ch - 1, tiles)),
            dma((n_ch - 1, tiles)),
        ],
        compiler_params=pltpu.CompilerParams(
            collective_id=0, has_side_effects=True, vmem_limit_bytes=67043328 - 4 * outs * steps
        ),
    )(trans, drive, back_drive, readout.reshape(2 * outs, readout.shape[2]))


def solution(mesh):
    in_specs = (
        P(None, "chan", "tm"),
        P(None, "chan", "tm"),
        P(None, "chan", "tm"),
        P("chan", None, None),
    )
    return jax.shard_map(
        functools.partial(on_device, mesh.shape["tm"], mesh.shape["chan"]),
        mesh=mesh,
        in_specs=in_specs,
        out_specs=P("chan", "tm"),
        check_vma=False,
    )
```
